8 devices in a mesh: dp: 2 (over z, y), tp: 4 (over x, core).
Axes of the slice: x: 2, y: 2, z: 1, core: 2. Of those that a mesh axis runs over, the one named last changes fastest.
Arguments:
- y_one: float32 [8, 576, 768], P('dp'), parts along dimension 0
- y_two: float32 [8, 576, 768], P('dp'), parts along dimension 0
- dy_one: float32 [8, 576, 768], P('dp'), parts along dimension 0
- dy_two: float32 [8, 576, 768], P('dp'), parts along dimension 0
- saved_one: float32 [3, 8, 576, 768], P(None, 'dp'), parts along dimension 1
- saved_two: float32 [3, 8, 576, 768], P(None, 'dp'), parts along dimension 1
- w_qkv: bfloat16 [7, 768, 3, 12, 64], P(None, None, None, 'tp')
- w_o: bfloat16 [7, 12, 64, 768], P(None, 'tp')
- w_in: bfloat16 [7, 768, 3072], P(None, None, 'tp')
- w_out: bfloat16 [7, 3072, 768], P(None, 'tp')
Outputs:
- output 1: float32 [8, 576, 768], P('dp'), parts along dimension 0
- output 2: float32 [8, 576, 768], P('dp'), parts along dimension 0
- output 3: float32 [8, 576, 768], P('dp'), parts along dimension 0
- output 4: float32 [8, 576, 768], P('dp'), parts along dimension 0
- output 5: float32 [14, 768, 3, 12, 64], P('dp', None, None, 'tp'), parts along dimension 0
- output 6: float32 [14, 12, 64, 768], P('dp', 'tp'), parts along dimension 0
- output 7: float32 [14, 768, 3072], P('dp', None, 'tp'), parts along dimension 0
- output 8: float32 [14, 3072, 768], P('dp', 'tp'), parts along dimension 0
There are 2 independent parts. The reference program is written for one: setup_inputs(seed, part) draws one part's arguments, and reference() takes and returns one part's arrays. A program takes and returns all parts, laid end to end along the dimension named above; an argument that names none is the same for every part.
All inputs are finite; a program needn't handle non-finite values.
Results may differ from the reference program's by a relative error of at most 0.0136928.
Values are sent between devices in bfloat16 or wider.
A program may use at most 1 GiB of HBM per device.

```python
import jax
import jax.numpy as jnp
from jax import lax

SEQS = 4
SEQ = 576
HIDDEN = 768
HEADS = 12
FF = 3072
PAIRS = 3

LAYERS = 2 * PAIRS + 1
HEAD = HIDDEN // HEADS
EPS = 1e-6


def setup_inputs(seed: int = 0, part: int = 0) -> dict:
    base_keys = jax.random.split(jax.random.key(seed), 2)
    act_keys = jax.random.split(jax.random.fold_in(base_keys[0], part), 6)
    w_keys = jax.random.split(base_keys[1], 4)
    state_shape = (SEQS, SEQ, HIDDEN)
    saved_shape = (PAIRS, SEQS, SEQ, HIDDEN)
    qk_gain = jnp.array([2.0 ** 0.5, 2.0 ** 0.5, 1.0], jnp.float32).reshape(1, 1, 3, 1, 1)
    wo_gain = 0.3 * (SEQ / 55.0) ** 0.5
    w_qkv = jax.random.normal(w_keys[0], (LAYERS, HIDDEN, 3, HEADS, HEAD), jnp.float32) * (HIDDEN ** -0.5) * qk_gain
    w_o = jax.random.normal(w_keys[1], (LAYERS, HEADS, HEAD, HIDDEN), jnp.float32) * (HIDDEN ** -0.5 * wo_gain)
    w_in = jax.random.normal(w_keys[2], (LAYERS, HIDDEN, FF), jnp.float32) * (HIDDEN ** -0.5)
    w_out = jax.random.normal(w_keys[3], (LAYERS, FF, HIDDEN), jnp.float32) * (0.45 * FF ** -0.5)
    return {
        "y_one": jax.random.normal(act_keys[0], state_shape, jnp.float32),
        "y_two": jax.random.normal(act_keys[1], state_shape, jnp.float32),
        "dy_one": jax.random.normal(act_keys[2], state_shape, jnp.float32),
        "dy_two": jax.random.normal(act_keys[3], state_shape, jnp.float32),
        "saved_one": jax.random.normal(act_keys[4], saved_shape, jnp.float32),
        "saved_two": jax.random.normal(act_keys[5], saved_shape, jnp.float32),
        "w_qkv": w_qkv.astype(jnp.bfloat16),
        "w_o": w_o.astype(jnp.bfloat16),
        "w_in": w_in.astype(jnp.bfloat16),
        "w_out": w_out.astype(jnp.bfloat16),
    }


def rms_norm(state):
    return state * lax.rsqrt(jnp.mean(state * state, axis=-1, keepdims=True) + EPS)


def to_bf(values):
    return values.astype(jnp.bfloat16).astype(jnp.float32)


def attend_one(qkv_one):
    q_one, k_one, v_one = qkv_one
    scores = jnp.einsum("qne,kne->nqk", q_one, k_one) * HEAD ** -0.5
    attn_probs = jax.nn.softmax(scores, axis=-1)
    return jnp.einsum("nqk,kne->qne", to_bf(attn_probs), v_one)


def branch_f(state, w_qkv, w_o):
    normed = to_bf(rms_norm(state))
    qkv_all = to_bf(jnp.einsum("bsh,hkne->kbsne", normed, w_qkv))
    heads_out = lax.map(jax.checkpoint(attend_one), (qkv_all[0], qkv_all[1], qkv_all[2]))
    return jnp.einsum("bsne,neh->bsh", to_bf(heads_out), w_o)


def branch_g(state, w_in, w_out):
    normed = to_bf(rms_norm(state))
    hidden = jnp.einsum("bsh,hf->bsf", normed, w_in)
    return jnp.einsum("bsf,fh->bsh", to_bf(jax.nn.gelu(hidden, approximate=True)), w_out)


def reversible_back(block_w, y_one, y_two, d_one, d_two):
    w_qkv, w_o, w_in, w_out = block_w
    g_val, g_pull = jax.vjp(branch_g, y_one, w_in, w_out)
    x_two = y_two - g_val
    g_dx, g_win, g_wout = g_pull(d_two)
    d_one = d_one + g_dx
    f_val, f_pull = jax.vjp(branch_f, x_two, w_qkv, w_o)
    x_one = y_one - f_val
    f_dx, f_wqkv, f_wo = f_pull(d_one)
    return x_one, x_two, d_one, d_two + f_dx, (f_wqkv, f_wo, g_win, g_wout)


def plain_back(block_w, x_one, x_two, d_one, d_two):
    w_qkv, w_o, w_in, w_out = block_w
    f_pull = jax.vjp(branch_f, x_two, w_qkv, w_o)[1]
    f_dx, f_wqkv, f_wo = f_pull(d_one)
    g_pull = jax.vjp(branch_g, x_one, w_in, w_out)[1]
    g_dx, g_win, g_wout = g_pull(d_two)
    return d_one + g_dx, d_two + f_dx, (f_wqkv, f_wo, g_win, g_wout)


def reference(y_one, y_two, dy_one, dy_two, saved_one, saved_two, w_qkv, w_o, w_in, w_out):
    weights = tuple(weight.astype(jnp.float32) for weight in (w_qkv, w_o, w_in, w_out))
    top_w = tuple(weight[LAYERS - 1] for weight in weights)
    x_one, x_two, d_one, d_two, top_grads = reversible_back(top_w, y_one, y_two, dy_one, dy_two)
    paired = tuple(weight[: 2 * PAIRS].reshape((PAIRS, 2) + weight.shape[1:]) for weight in weights)
    rev_w = tuple(weight[:, 0] for weight in paired)
    plain_w = tuple(weight[:, 1] for weight in paired)

    def pair_step(carry_in, scan_in):
        rev_block_w, plain_block_w, s_one, s_two = scan_in
        d_mid_one, d_mid_two, plain_grads = plain_back(plain_block_w, s_one, s_two, carry_in[2], carry_in[3])
        carry_out = reversible_back(rev_block_w, s_one, s_two, d_mid_one, d_mid_two)
        return carry_out[:4], (carry_out[4], plain_grads)

    final_state, scan_grads = lax.scan(pair_step, (x_one, x_two, d_one, d_two), (rev_w, plain_w, saved_one, saved_two), reverse=True)
    grad_out = tuple(
        jnp.concatenate([jnp.stack([rev_g, plain_g], axis=1).reshape((2 * PAIRS,) + rev_g.shape[1:]), top_g[None]], axis=0)
        for rev_g, plain_g, top_g in zip(scan_grads[0], scan_grads[1], top_grads)
    )
    return (final_state[0], final_state[1], final_state[2], final_state[3], grad_out[0], grad_out[1], grad_out[2], grad_out[3])
```

```python
import functools
import math

import jax
import jax.numpy as jnp
from jax import lax
from jax.experimental import pallas as pl
from jax.experimental.pallas import tpu as pltpu
from jax.sharding import PartitionSpec as P

EPS = 1e-6
BF = jnp.bfloat16
F32 = jnp.float32
GELU_C = math.sqrt(2.0 / math.pi)
ROWS = 32


def mm(lhs, rhs, lhs_dim, rhs_dim):
    return lax.dot_general(lhs, rhs, (((lhs_dim,), (rhs_dim,)), ((), ())), preferred_element_type=F32)


def shape(dims, dtype):
    return jax.ShapeDtypeStruct(dims, dtype)


def kernel_call(body, name, ins, outs, scratch=(), after=(), any_in=(), any_out=(), alias=None, flops=0, vmem=32 << 20):
    n_in, n_after = len(ins), len(after)

    def wrapped(*refs):
        body(refs[:n_in], refs[n_in + n_after :])

    in_specs = [pl.BlockSpec(memory_space=pl.ANY if idx in any_in else pltpu.VMEM) for idx in range(n_in)]
    in_specs += [pl.BlockSpec(memory_space=pl.ANY)] * n_after
    out_specs = [pl.BlockSpec(memory_space=pl.ANY if idx in any_out else pltpu.VMEM) for idx in range(len(outs))]
    moved = sum(math.prod(arr.shape) * arr.dtype.itemsize for arr in list(ins) + list(outs))
    return pl.pallas_call(
        wrapped,
        out_shape=list(outs),
        in_specs=in_specs,
        out_specs=out_specs,
        scratch_shapes=list(scratch),
        input_output_aliases=alias or {},
        compiler_params=pltpu.CompilerParams(vmem_limit_bytes=vmem),
        cost_estimate=pl.CostEstimate(flops=flops, bytes_accessed=moved, transcendentals=0),
        name=name,
    )(*ins, *after)


def inv_rms(x):
    return lax.rsqrt(jnp.mean(x * x, axis=-1, keepdims=True) + EPS)


def pull_norm(x, grad):
    inv = inv_rms(x)
    return inv * (grad - x * (inv * inv * jnp.mean(grad * x, axis=-1, keepdims=True)))


def gelu_and_slope(hid):
    sq = hid * hid
    tanh = jnp.tanh(hid * (GELU_C + (GELU_C * 0.044715) * sq))
    half = 0.5 * hid
    act = half + half * tanh
    slope = (0.5 + 0.5 * tanh) + (half - half * (tanh * tanh)) * (GELU_C + (3.0 * GELU_C * 0.044715) * sq)
    return act, slope


class Cotangent:
    def __init__(self, value):
        self.value, self.pending, self.bf = value, None, None

    def add(self, mine, recv):
        assert self.pending is None
        self.pending, self.bf = (mine, recv), None

    def operands(self):
        if self.bf is not None:
            return [self.bf], []
        out = [shape(self.value.shape, BF)]
        if self.pending is None:
            return [self.value], out
        return [self.value, *self.pending], out + [shape(self.value.shape, F32)]

    def settle(self, made):
        if made:
            self.bf = made[0]
        if len(made) == 2:
            self.value, self.pending = made[1], None


def read_cotangent(in_refs, out_refs):
    if not out_refs:
        return in_refs[0]
    if len(in_refs) == 1:
        out_refs[0][...] = in_refs[0][...].astype(BF)
    else:
        total = in_refs[0][...] + (in_refs[1][...].astype(F32) + in_refs[2][...].astype(F32))
        out_refs[1][...] = total
        out_refs[0][...] = total.astype(BF)
    return out_refs[0]


def attn_body(n_d_in, n_d_out, ins, rest):
    x_ref = ins[0]
    wq_own, wq_par, wo_own, wo_par = ins[1 + n_d_in :]
    t_ref, a_ref, dqkv_ref, o_ref = rest[:4]
    d_ref = read_cotangent(ins[1 : 1 + n_d_in], rest[4 : 4 + n_d_out])
    qkv_ref, do_ref, s_ref, dp_ref, pb_ref, ds_ref = rest[4 + n_d_out :]
    tokens = x_ref.shape[0]
    wide = wo_own.shape[0]
    both = 2 * wide
    x = x_ref[...]
    a_ref[...] = (x * inv_rms(x)).astype(BF)
    w_all = jnp.concatenate([ref[part * wide : (part + 1) * wide, :] for part in range(3) for ref in (wq_own, wq_par)], axis=0)
    qkv = mm(a_ref[...], w_all, 1, 1)
    qkv_ref[:, :both] = qkv[:, :both].astype(BF) * jnp.asarray(0.125, BF)
    qkv_ref[:, both:] = qkv[:, both:].astype(BF)
    do_ref[...] = mm(d_ref[...], jnp.concatenate([wo_own[...], wo_par[...]], axis=0), 1, 1).astype(BF)
    lane = lax.broadcasted_iota(jnp.int32, (tokens, 128), 1)
    for pair in range(both // 128):
        cols = slice(pair * 128, pair * 128 + 128)
        q_two = qkv_ref[:, cols]
        k_two = qkv_ref[:, both + pair * 128 : both + pair * 128 + 128]
        v_two = qkv_ref[:, 2 * both + pair * 128 : 2 * both + pair * 128 + 128]
        do_two = do_ref[:, cols]
        sums = []
        for head in range(2):
            keep = (lane < 64) if head == 0 else (lane >= 64)
            zero = jnp.zeros_like(q_two)
            s_ref[head] = mm(jnp.where(keep, q_two, zero), k_two, 1, 1)
            dp_ref[head] = mm(jnp.where(keep, do_two, zero), v_two, 1, 1)
            for row in range(0, tokens, ROWS):
                rows = slice(row, row + ROWS)
                scores = s_ref[head, rows, :]
                d_probs = dp_ref[head, rows, :]
                exps = jnp.exp(scores - jnp.max(scores, axis=-1, keepdims=True))
                probs = exps * (1.0 / jnp.sum(exps, axis=-1, keepdims=True))
                pb_ref[head, rows, :] = probs.astype(BF)
                ds_ref[head, rows, :] = (probs * (d_probs - jnp.sum(d_probs * probs, axis=-1, keepdims=True))).astype(BF)
            sums.append(
                (
                    mm(pb_ref[head], v_two, 1, 0),
                    mm(ds_ref[head], k_two, 1, 0),
                    mm(ds_ref[head], q_two, 0, 0),
                    mm(pb_ref[head], do_two, 0, 0),
                )
            )
        heads, d_q, d_k, d_v = (jnp.where(lane < 64, low, high) for low, high in zip(*sums))
        o_ref[:, cols] = heads.astype(BF)
        dqkv_ref[:, cols] = (d_q * 0.125).astype(BF)
        dqkv_ref[:, both + pair * 128 : both + pair * 128 + 128] = d_k.astype(BF)
        dqkv_ref[:, 2 * both + pair * 128 : 2 * both + pair * 128 + 128] = d_v.astype(BF)
    d_normed = mm(dqkv_ref[...], w_all, 1, 0)
    t_ref[...] = pull_norm(x_ref[...], d_normed).astype(BF)


def attn_step(x, cot, weights, after):
    d_in, d_out = cot.operands()
    tokens, hidden = x.shape
    both = 2 * weights[2].shape[0]
    outs = [shape((tokens, hidden), BF), shape((tokens, hidden), BF), shape((tokens, 3 * both), BF), shape((tokens, both), BF)] + d_out
    scratch = [
        pltpu.VMEM((tokens, 3 * both), BF),
        pltpu.VMEM((tokens, both), BF),
        pltpu.VMEM((2, tokens, tokens), F32),
        pltpu.VMEM((2, tokens, tokens), F32),
        pltpu.VMEM((2, tokens, tokens), BF),
        pltpu.VMEM((2, tokens, tokens), BF),
    ]
    flops = 2 * tokens * hidden * 7 * both + 12 * tokens * tokens * 256 * (both // 64)
    made = kernel_call(
        functools.partial(attn_body, len(d_in), len(d_out)), "attn_back", [x, *d_in, *weights], outs, scratch, after, flops=flops
    )
    cot.settle(made[4:])
    return made[:4]


def mlp_body(n_d_in, n_d_out, has_acc, last, ins, rest):
    x_ref = ins[0]
    win_own, win_par, wout_own, wout_par = ins[1 + n_d_in : 5 + n_d_in]
    t_ref, a_ref, act_own, act_par, dh_own, dh_par = rest[:6]
    d_ref = read_cotangent(ins[1 : 1 + n_d_in], rest[6 : 6 + n_d_out])
    x = x_ref[...]
    a_ref[...] = (x * inv_rms(x)).astype(BF)
    width = win_own.shape[1]
    step = 256
    for win, wout, act_ref, dh_ref in ((win_own, wout_own, act_own, dh_own), (win_par, wout_par, act_par, dh_par)):
        for col in range(0, width, step):
            cols = slice(col, col + step)
            act, slope = gelu_and_slope(mm(a_ref[...], win[:, cols], 1, 0))
            act_ref[:, cols] = act.astype(BF)
            dh_ref[:, cols] = (mm(d_ref[...], wout[cols, :], 1, 1) * slope).astype(BF)
    d_normed = mm(
        jnp.concatenate([dh_own[...], dh_par[...]], axis=1), jnp.concatenate([win_own[...], win_par[...]], axis=1), 1, 1
    )
    part = pull_norm(x_ref[...], d_normed)
    if has_acc:
        part = part + ins[5 + n_d_in][...]
    t_ref[...] = part.astype(t_ref.dtype)


def mlp_step(x, cot, weights, acc, last, after):
    d_in, d_out = cot.operands()
    tokens, hidden = x.shape
    width = weights[0].shape[1]
    outs = [shape((tokens, hidden), BF if last else F32), shape((tokens, hidden), BF)] + [shape((tokens, width), BF)] * 4 + d_out
    ins = [x, *d_in, *weights] + ([] if acc is None else [acc])
    made = kernel_call(
        functools.partial(mlp_body, len(d_in), len(d_out), acc is not None, last),
        "mlp_back",
        ins,
        outs,
        (),
        after,
        flops=12 * tokens * hidden * width,
    )
    cot.settle(made[6:])
    return made[:6]


def rebuild_body(ins, rest):
    x_ref, y_ref = ins[:2]
    win, wout = ins[2:6], ins[6:10]
    out_ref, a_ref, act_ref = rest
    x = x_ref[...]
    a_ref[...] = (x * inv_rms(x)).astype(BF)
    width = win[0].shape[1]
    step = 256
    for shard in range(4):
        for col in range(0, width, step):
            act, _ = gelu_and_slope(mm(a_ref[...], win[shard][:, col : col + step], 1, 0))
            act_ref[:, shard * width + col : shard * width + col + step] = act.astype(BF)
    parts = [
        mm(act_ref[:, 2 * pair * width : 2 * (pair + 1) * width], jnp.concatenate([wout[2 * pair][...], wout[2 * pair + 1][...]], axis=0), 1, 0)
        for pair in range(2)
    ]
    out_ref[...] = y_ref[...] - (parts[0] + parts[1])


def rebuild_step(x, y, win, wout, after):
    tokens, hidden = x.shape
    width = win[0].shape[1]
    scratch = [pltpu.VMEM((tokens, hidden), BF), pltpu.VMEM((tokens, 4 * width), BF)]
    return kernel_call(
        rebuild_body, "rebuild", [x, y, *win, *wout], [shape(x.shape, F32)], scratch, after, flops=16 * tokens * hidden * width
    )[0]


def attn_out_body(ins, rest):
    y_ref, heads, heads_far, wo = ins[0], ins[1], ins[2], ins[3:]
    near = mm(heads[...], jnp.concatenate([wo[0][...], wo[1][...]], axis=0), 1, 0)
    far = mm(heads_far[...], jnp.concatenate([wo[2][...], wo[3][...]], axis=0), 1, 0)
    rest[0][...] = y_ref[...] - (near + far)


def attn_out_step(y, heads, heads_far, wo, after):
    return kernel_call(
        attn_out_body, "attn_out", [y, heads, heads_far, *wo], [shape(y.shape, F32)], (), after, flops=4 * y.shape[0] * y.shape[1] * heads.shape[1]
    )[0]


def rows_of(refs):
    return jnp.concatenate([ref[...] for ref in refs], axis=0)


def attn_dw(half, wide, refs):
    a, dqkv, heads, d_bf = refs[0:2], refs[2:4], refs[4:6], refs[6:8]

    def picked(pair, base):
        start = base + (0 if half == 0 else 128)
        moved = jnp.concatenate([ref[:, start : start + 256] for ref in pair], axis=0).T
        return moved[:wide] if half == 0 else moved[256 - wide :]

    left = jnp.concatenate([picked(dqkv, part * 2 * wide) for part in range(3)], axis=0)
    return mm(left, rows_of(a), 1, 0), mm(picked(heads, 0), rows_of(d_bf), 1, 0)


def mlp_dw(refs):
    a, dh, act, d_bf = refs[0:2], refs[2:4], refs[4:6], refs[6:8]
    return mm(rows_of(a), rows_of(dh), 0, 0), mm(rows_of(act), rows_of(d_bf), 0, 0)


def dw_theirs_body(sums, ins, rest):
    for ref, value in zip(rest, sums(ins)):
        ref[...] = value


def dw_mine_body(sums, layer, ins, rest):
    stacks, bufs, sems = rest[:2], rest[2:4], rest[4]
    copies = []
    for idx, value in enumerate(sums(ins[:8])):
        bufs[idx][...] = value + ins[8 + idx][...]
        copy = pltpu.make_async_copy(bufs[idx], stacks[idx].at[layer], sems.at[idx])
        copy.start()
        copies.append(copy)
    for copy in copies:
        copy.wait()


def dw_theirs(sums, name, ins, outs, after, flops):
    return kernel_call(functools.partial(dw_theirs_body, sums), name, ins, outs, (), after, flops=flops)


def dw_mine(sums, name, layer, layers, ins, recv, stacks, after, flops):
    outs = [shape((layers,) + part.shape, F32) for part in recv]
    full = list(ins) + list(recv) + (list(stacks) if stacks else [])
    alias = {10: 0, 11: 1} if stacks else {}
    scratch = [pltpu.VMEM(part.shape, F32) for part in recv] + [pltpu.SemaphoreType.DMA((2,))]
    return kernel_call(
        functools.partial(dw_mine_body, sums, layer),
        name,
        full,
        outs,
        scratch,
        after,
        any_in=(10, 11),
        any_out=(0, 1),
        alias=alias,
        flops=flops,
    )


def solution(mesh):
    act_spec = P("dp", None, None)
    saved_spec = P(None, "dp", None, None)
    weight_specs = (P(None, None, None, "tp", None), P(None, "tp", None, None), P(None, None, "tp"), P(None, "tp", None))
    grad_specs = (P("dp", None, None, "tp", None), P("dp", "tp", None, None), P("dp", None, "tp"), P("dp", "tp", None))
    across = [(0, 2), (2, 0), (1, 3), (3, 1)]
    partner = [(0, 1), (1, 0), (2, 3), (3, 2)]

    def per_device(y_one, y_two, dy_one, dy_two, saved_one, saved_two, w_qkv, w_o, w_in, w_out):
        layers, pairs = w_qkv.shape[0], saved_one.shape[0]
        tokens, hidden = y_one.shape[1:]
        core = lax.rem(lax.axis_index("tp"), 2)

        def far(value):
            return lax.ppermute(value, "tp", across)

        def near(value):
            return lax.ppermute(value, "tp", partner)

        def mine(whole, seq):
            return lax.dynamic_index_in_dim(whole, 2 * core + seq, 0, keepdims=False)

        wq_t = jnp.transpose(w_qkv, (0, 2, 3, 4, 1)).reshape(layers, -1, hidden)
        wo_r = w_o.reshape(layers, -1, hidden)
        wide = wo_r.shape[1]

        mlp_w, attn_w, far_w = {}, {}, {}
        top = layers - 1

        def fetch_mlp(layer):
            own_in, own_out = w_in[layer], w_out[layer]
            mlp_w[layer] = (own_in, near(own_in), own_out, near(own_out))

        def fetch_attn(layer):
            own_q, own_o = wq_t[layer], wo_r[layer]
            attn_w[layer] = (own_q, near(own_q), own_o, near(own_o))

        def fetch_far(layer):
            far_in, far_out = far(w_in[layer]), far(w_out[layer])
            far_w[layer] = (far_in, near(far_in), far_out, near(far_out))

        for layer in reversed(range(layers)):
            fetch_mlp(layer)
            fetch_attn(layer)
            if layer % 2 == 0:
                fetch_far(layer)

        last = [()]

        def run(step, *args):
            made = step(*args, last[0])
            last[0] = ((made[0] if isinstance(made, (list, tuple)) else made),)
            return made

        d_one = [Cotangent(mine(dy_one, seq)) for seq in range(2)]
        d_two = [Cotangent(mine(dy_two, seq)) for seq in range(2)]
        in_one, in_two, x_two = {}, {}, {}
        for seq in range(2):
            in_one[pairs, seq] = mine(y_one, seq)
            in_two[pairs, seq] = mine(y_two, seq)
            for pair in range(pairs):
                in_one[pair, seq] = mine(saved_one[pair], seq)
                in_two[pair, seq] = mine(saved_two[pair], seq)

        attn_parts, mlp_parts = {}, {}
        acc = {}

        def attn(layer, seq):
            x = x_two[layer, seq] if layer % 2 == 0 else in_two[layer // 2, seq]
            part, a, dqkv, heads = run(attn_step, x, d_one[seq], attn_w[layer])
            attn_parts[layer, seq] = (a, dqkv, heads, d_one[seq].bf)
            return part, far(part)

        def mlp(layer, seq):
            pair = layer // 2
            reversible = layer % 2 == 0
            part, a, act_own, act_par, dh_own, dh_par = run(
                mlp_step, in_one[pair, seq], d_two[seq], mlp_w[layer], acc.get(seq) if reversible else None, reversible
            )
            mlp_parts[layer, seq] = (a, (dh_own, dh_par), (act_own, act_par), d_two[seq].bf)
            if not reversible:
                acc[seq] = part
                return None
            return part, far(part)

        def rebuild(layer, seq):
            pair = layer // 2
            own_in, par_in, own_out, par_out = mlp_w[layer]
            far_in, far_in_par, far_out, far_out_par = far_w[layer]
            x_two[layer, seq] = run(
                rebuild_step,
                in_one[pair, seq],
                in_two[pair, seq],
                (own_in, par_in, far_in, far_in_par),
                (own_out, par_out, far_out, far_out_par),
            )

        stacks = {"attn": None, "mlp": None}
        sent = {}

        def attn_grads(layer):
            parts = [attn_parts[layer, seq] for seq in range(2)]
            ins = [parts[seq][slot] for slot in range(4) for seq in range(2)]
            outs = [shape((3 * wide, hidden), F32), shape((wide, hidden), F32)]
            flops = 16 * tokens * hidden * wide
            theirs = run(dw_theirs, functools.partial(attn_dw, 1, wide), "attn_dw_theirs", ins, outs) if False else None
            made = dw_theirs(functools.partial(attn_dw, 1, wide), "attn_dw_theirs", ins, outs, last[0], flops)
            last[0] = (made[0],)
            sent["attn", layer] = (ins, [near(value) for value in made], flops)

        def attn_grads_end(layer):
            ins, recv, flops = sent["attn", layer]
            stacks["attn"] = dw_mine(
                functools.partial(attn_dw, 0, wide), "attn_dw_mine", layer, layers, ins, recv, stacks["attn"], last[0], flops
            )

        def mlp_grads(layer):
            parts = [mlp_parts[layer, seq] for seq in range(2)]

            def operands(half):
                return (
                    [parts[seq][0] for seq in range(2)]
                    + [parts[seq][1][half] for seq in range(2)]
                    + [parts[seq][2][half] for seq in range(2)]
                    + [parts[seq][3] for seq in range(2)]
                )

            width = w_in.shape[2]
            outs = [shape((hidden, width), F32), shape((width, hidden), F32)]
            flops = 8 * tokens * hidden * width
            made = dw_theirs(mlp_dw, "mlp_dw_theirs", operands(1), outs, last[0], flops)
            last[0] = (made[0],)
            sent["mlp", layer] = (operands(0), [near(value) for value in made], flops)

        def mlp_grads_end(layer):
            ins, recv, flops = sent["mlp", layer]
            stacks["mlp"] = dw_mine(mlp_dw, "mlp_dw_mine", layer, layers, ins, recv, stacks["mlp"], last[0], flops)

        for seq in range(2):
            d_one[seq].add(*mlp(top, seq))
        for seq in range(2):
            rebuild(top, seq)
        mlp_grads(top)
        heads = {}
        for pair in reversed(range(pairs + 1)):
            layer = 2 * pair
            for seq in range(2):
                one = attn(layer, seq)
                if pair:
                    two = attn(layer - 1, seq)
                    d_two[seq].add(*one)
                    d_two_next = two
                    heads[seq] = d_two_next
                else:
                    d_two[seq].add(*one)
            mlp_grads_end(layer)
            if pair == 0:
                break
            rebuild(layer - 2, 0)
            mlp(layer - 1, 0)
            d_two[0].add(*heads[0])
            d_one[0].add(*mlp(layer - 2, 0))
            rebuild(layer - 2, 1)
            attn_grads(layer)
            mlp(layer - 1, 1)
            d_two[1].add(*heads[1])
            attn_grads(layer - 1)
            attn_grads_end(layer)
            d_one[1].add(*mlp(layer - 2, 1))
            attn_grads_end(layer - 1)
            mlp_grads(layer - 1)
            mlp_grads(layer - 2)
            mlp_grads_end(layer - 1)
        attn_grads(0)
        wo_own, wo_par = attn_w[0][2:]
        wo_all = (wo_own, wo_par, far(wo_own), far(wo_par))
        x_one = []
        for seq in range(2):
            own = attn_parts[0, seq][2]
            x_one.append(attn_out_step(in_one[0, seq], own, far(own), wo_all, last[0]))
        attn_grads_end(0)
        finals = [x_one, [x_two[0, seq] for seq in range(2)], [d_one[seq].value for seq in range(2)], []]
        for seq in range(2):
            own, recv = d_two[seq].pending
            finals[3].append(d_two[seq].value + (own.astype(F32) + recv.astype(F32)))

        def whole(two):
            own = jnp.stack(two)
            other = near(own)
            return jnp.where(core == 0, jnp.concatenate([own, other]), jnp.concatenate([other, own]))

        dwq, dwo = stacks["attn"]
        dwin, dwout = stacks["mlp"]
        dwq = jnp.transpose(dwq.reshape((layers,) + w_qkv.shape[2:] + (hidden,)), (0, 4, 1, 2, 3))
        return tuple(whole(two) for two in finals) + (dwq, dwo.reshape(w_o.shape), dwin, dwout)

    return jax.shard_map(
        per_device,
        mesh=mesh,
        in_specs=(act_spec,) * 4 + (saved_spec,) * 2 + weight_specs,
        out_specs=(act_spec,) * 4 + grad_specs,
        check_vma=False,
    )
```

```python
import functools
import math

import jax
import jax.numpy as jnp
from jax import lax
from jax.experimental import pallas as pl
from jax.experimental.pallas import tpu as pltpu
from jax.sharding import PartitionSpec as P

EPS = 1e-6
BF = jnp.bfloat16
F32 = jnp.float32
GELU_C = math.sqrt(2.0 / math.pi)
ROWS = 32
COPIES = 48


def mm(lhs, rhs, lhs_dim, rhs_dim):
    return lax.dot_general(lhs, rhs, (((lhs_dim,), (rhs_dim,)), ((), ())), preferred_element_type=F32)


class In:
    def __init__(self, arr, dims=None, at=None, other=None):
        self.arr, self.other = arr, other
        self.dims = tuple(dims or arr.shape)
        self.at = at or (lambda ref, first: ref)


class Out:
    def __init__(self, dims, dtype, full=None, at=None, into=None):
        self.dims, self.dtype = tuple(dims), dtype
        self.full = tuple(full or dims)
        self.at = at or (lambda ref, first: ref)
        self.into = into


class Moves:
    def __init__(self, sems):
        self.sems, self.used, self.open, self.loads = sems, 0, [], {}

    def copy(self, src, dst):
        made = pltpu.make_async_copy(src, dst, self.sems.at[self.used])
        self.used += 1
        return made

    def load(self, idx, sources, pick, dst):
        if len(sources) == 1:
            copy = self.copy(sources[0], dst)
            copy.start()
        else:
            sem = self.sems.at[self.used]
            self.used += 1
            copy = pltpu.make_async_copy(sources[0], dst, sem)
            pl.when(pick == 0)(copy.start)
            pl.when(pick == 1)(pltpu.make_async_copy(sources[1], dst, sem).start)
        self.loads[idx] = (copy, dst)

    def get(self, idx):
        copy, dst = self.loads[idx]
        if copy is not None:
            copy.wait()
            self.loads[idx] = (None, dst)
        return dst

    def store(self, src, dst):
        copy = self.copy(src, dst)
        copy.start()
        self.open.append(copy)

    def finish(self):
        for copy in self.open:
            copy.wait()


def kernel_call(body, name, where, ins, outs, scratch=(), after=(), flops=0):
    arrays, slots, alias = [], [], {}
    for item in ins:
        slots.append([len(arrays) + 1] + ([len(arrays) + 2] if item.other is not None else []))
        arrays += [item.arr] + ([item.other] if item.other is not None else [])
    for idx, item in enumerate(outs):
        if item.into is not None:
            alias[len(arrays) + 1] = idx
            arrays.append(item.into)
    arrays += list(after)
    n_arrays = len(arrays) + 1

    def wrapped(*refs):
        where_ref, out_refs = refs[0], refs[n_arrays : n_arrays + len(outs)]
        rest = refs[n_arrays + len(outs) :]
        in_bufs, out_bufs = rest[: len(ins)], rest[len(ins) : len(ins) + len(outs)]
        moves = Moves(rest[-1])
        first, pick = where_ref[0], where_ref[1]
        for idx, item in enumerate(ins):
            moves.load(idx, [item.at(refs[slot], first) for slot in slots[idx]], pick, in_bufs[idx])

        def storer(idx):
            def store(rows=None, src=None, at=None):
                dst = (at or outs[idx].at)(out_refs[idx], first)
                src = out_bufs[idx] if src is None else src
                if rows is not None:
                    src, dst = src.at[rows], dst.at[rows]
                moves.store(src, dst)

            return store

        body(moves.get, [(out_bufs[idx], storer(idx)) for idx in range(len(outs))], rest[len(ins) + len(outs) : -1])
        moves.finish()

    anywhere = pl.BlockSpec(memory_space=pl.ANY)
    moved = sum(math.prod(item.dims) * item.arr.dtype.itemsize for item in ins)
    moved += sum(math.prod(item.dims) * jnp.dtype(item.dtype).itemsize for item in outs)
    return pl.pallas_call(
        wrapped,
        out_shape=[jax.ShapeDtypeStruct(item.full, item.dtype) for item in outs],
        in_specs=[pl.BlockSpec(memory_space=pltpu.SMEM)] + [anywhere] * len(arrays),
        out_specs=[anywhere] * len(outs),
        scratch_shapes=[pltpu.VMEM(item.dims, item.arr.dtype) for item in ins]
        + [pltpu.VMEM(item.dims, item.dtype) for item in outs]
        + list(scratch)
        + [pltpu.SemaphoreType.DMA((COPIES,))],
        input_output_aliases=alias,
        compiler_params=pltpu.CompilerParams(vmem_limit_bytes=60 << 20),
        cost_estimate=pl.CostEstimate(flops=flops, bytes_accessed=moved, transcendentals=0),
        name=name,
    )(where, *arrays)


def inv_rms(x):
    return lax.rsqrt(jnp.mean(x * x, axis=-1, keepdims=True) + EPS)


def pull_norm(x, grad):
    inv = inv_rms(x)
    return inv * (grad - x * (inv * inv * jnp.mean(grad * x, axis=-1, keepdims=True)))


def gelu(hid):
    half = 0.5 * hid
    return half + half * jnp.tanh(hid * (GELU_C + (GELU_C * 0.044715) * (hid * hid)))


def gelu_and_slope(hid):
    sq = hid * hid
    tanh = jnp.tanh(hid * (GELU_C + (GELU_C * 0.044715) * sq))
    half = 0.5 * hid
    act = half + half * tanh
    slope = (0.5 + 0.5 * tanh) + (half - half * (tanh * tanh)) * (GELU_C + (3.0 * GELU_C * 0.044715) * sq)
    return act, slope


class Cotangent:
    def __init__(self, value, dims):
        self.value, self.dims, self.pending, self.bf = value, dims, None, None

    def add(self, mine, recv):
        assert self.pending is None
        self.pending, self.bf = (In(mine), In(recv)), None

    def operands(self):
        if self.bf is not None:
            return [self.bf], []
        if self.pending is None:
            return [self.value], [Out(self.dims, BF)]
        return [self.value, *self.pending], [Out(self.dims, BF), Out(self.dims, F32)]

    def settle(self, made):
        if made:
            self.bf = In(made[0])
        if len(made) == 2:
            self.value, self.pending = In(made[1]), None


def read_cotangent(refs, puts):
    if not puts:
        return refs[0]
    if len(refs) == 1:
        puts[0][0][...] = refs[0][...].astype(BF)
    else:
        total = refs[0][...] + (refs[1][...].astype(F32) + refs[2][...].astype(F32))
        puts[1][0][...] = total
        puts[0][0][...] = total.astype(BF)
    for _, store in puts:
        store()
    return puts[0][0]


def attn_body(n_d, get, put, scratch):
    (t_ref, t_store), (a_ref, a_store), (dqkv_ref, dqkv_store), (o_ref, o_store) = put[:4]
    qkv_ref, do_ref, s_ref, dp_ref, pb_ref, ds_ref = scratch
    x_ref = get(0)
    tokens = x_ref.shape[0]
    x = x_ref[...]
    a_ref[...] = (x * inv_rms(x)).astype(BF)
    a_store()
    wq_own, wq_par = get(1 + n_d), get(2 + n_d)
    wide = wq_own.shape[0] // 3
    both = 2 * wide
    w_all = jnp.concatenate([ref[part * wide : (part + 1) * wide, :] for part in range(3) for ref in (wq_own, wq_par)], axis=0)
    qkv = mm(a_ref[...], w_all, 1, 1)
    qkv_ref[:, :both] = qkv[:, :both].astype(BF) * jnp.asarray(0.125, BF)
    qkv_ref[:, both:] = qkv[:, both:].astype(BF)
    d_ref = read_cotangent([get(1 + idx) for idx in range(n_d)], put[4:])
    wo_own, wo_par = get(3 + n_d), get(4 + n_d)
    do_ref[...] = mm(d_ref[...], jnp.concatenate([wo_own[...], wo_par[...]], axis=0), 1, 1).astype(BF)
    lane = lax.broadcasted_iota(jnp.int32, (tokens, 128), 1)
    for pair in range(both // 128):
        cols = slice(pair * 128, pair * 128 + 128)
        q_two = qkv_ref[:, cols]
        k_two = qkv_ref[:, both + pair * 128 : both + pair * 128 + 128]
        v_two = qkv_ref[:, 2 * both + pair * 128 : 2 * both + pair * 128 + 128]
        do_two = do_ref[:, cols]
        sums = []
        for head in range(2):
            keep = (lane < 64) if head == 0 else (lane >= 64)
            zero = jnp.zeros_like(q_two)
            s_ref[head] = mm(jnp.where(keep, q_two, zero), k_two, 1, 1)
            dp_ref[head] = mm(jnp.where(keep, do_two, zero), v_two, 1, 1)
            for row in range(0, tokens, ROWS):
                rows = slice(row, row + ROWS)
                scores = s_ref[head, rows, :]
                d_probs = dp_ref[head, rows, :]
                exps = jnp.exp(scores - jnp.max(scores, axis=-1, keepdims=True))
                probs = exps * (1.0 / jnp.sum(exps, axis=-1, keepdims=True))
                pb_ref[head, rows, :] = probs.astype(BF)
                ds_ref[head, rows, :] = (probs * (d_probs - jnp.sum(d_probs * probs, axis=-1, keepdims=True))).astype(BF)
            sums.append(
                (
                    mm(pb_ref[head], v_two, 1, 0),
                    mm(ds_ref[head], k_two, 1, 0),
                    mm(ds_ref[head], q_two, 0, 0),
                    mm(pb_ref[head], do_two, 0, 0),
                )
            )
        heads, d_q, d_k, d_v = (jnp.where(lane < 64, low, high) for low, high in zip(*sums))
        o_ref[:, cols] = heads.astype(BF)
        dqkv_ref[:, cols] = (d_q * 0.125).astype(BF)
        dqkv_ref[:, both + pair * 128 : both + pair * 128 + 128] = d_k.astype(BF)
        dqkv_ref[:, 2 * both + pair * 128 : 2 * both + pair * 128 + 128] = d_v.astype(BF)
    o_store()
    dqkv_store()
    d_normed = mm(dqkv_ref[...], w_all, 1, 0)
    t_ref[...] = pull_norm(x_ref[...], d_normed).astype(BF)
    t_store()


def attn_step(where, x, cot, weights, after):
    d_in, d_out = cot.operands()
    tokens, hidden = x.dims
    both = 2 * weights[2].dims[0]
    outs = [Out((tokens, hidden), BF), Out((tokens, hidden), BF), Out((tokens, 3 * both), BF), Out((tokens, both), BF)] + d_out
    scratch = [
        pltpu.VMEM((tokens, 3 * both), BF),
        pltpu.VMEM((tokens, both), BF),
        pltpu.VMEM((2, tokens, tokens), F32),
        pltpu.VMEM((2, tokens, tokens), F32),
        pltpu.VMEM((2, tokens, tokens), BF),
        pltpu.VMEM((2, tokens, tokens), BF),
    ]
    flops = 2 * tokens * hidden * 7 * both + 12 * tokens * tokens * 256 * (both // 64)
    made = kernel_call(
        functools.partial(attn_body, len(d_in)), "attn_back", where, [x, *d_in, *weights], outs, scratch, after, flops=flops
    )
    cot.settle(made[4:])
    return made[:4]


def mlp_body(n_d, has_acc, get, put, scratch):
    (t_ref, t_store), (a_ref, a_store) = put[:2]
    acts, dhs = put[2:4], put[4:6]
    x_ref = get(0)
    x = x_ref[...]
    a_ref[...] = (x * inv_rms(x)).astype(BF)
    a_store()
    d_ref = read_cotangent([get(1 + idx) for idx in range(n_d)], put[6:])
    step = 256
    wins = []
    for half in range(2):
        win, wout = get(1 + n_d + 2 * half), get(2 + n_d + 2 * half)
        wins.append(win)
        for col in range(0, win.shape[1], step):
            cols = slice(col, col + step)
            act, slope = gelu_and_slope(mm(a_ref[...], win[:, cols], 1, 0))
            acts[half][0][:, cols] = act.astype(BF)
            dhs[half][0][:, cols] = (mm(d_ref[...], wout[cols, :], 1, 1) * slope).astype(BF)
        acts[half][1]()
        dhs[half][1]()
    d_normed = mm(
        jnp.concatenate([dhs[0][0][...], dhs[1][0][...]], axis=1), jnp.concatenate([wins[0][...], wins[1][...]], axis=1), 1, 1
    )
    part = pull_norm(x_ref[...], d_normed)
    if has_acc:
        part = part + get(5 + n_d)[...]
    t_ref[...] = part.astype(t_ref.dtype)
    t_store()


def mlp_step(where, x, cot, weights, acc, last, after):
    d_in, d_out = cot.operands()
    tokens, hidden = x.dims
    width = weights[0].dims[1]
    outs = [Out((tokens, hidden), BF if last else F32), Out((tokens, hidden), BF)] + [Out((tokens, width), BF)] * 4 + d_out
    ins = [x, *d_in, *weights] + ([] if acc is None else [In(acc)])
    made = kernel_call(
        functools.partial(mlp_body, len(d_in), acc is not None),
        "mlp_back",
        where,
        ins,
        outs,
        (),
        after,
        flops=12 * tokens * hidden * width,
    )
    cot.settle(made[6:])
    return made[:6]


def rebuild_body(get, put, scratch):
    (out_ref, out_store), (a_ref, act_ref) = put[0], scratch
    x = get(0)[...]
    a_ref[...] = (x * inv_rms(x)).astype(BF)
    step = 256
    parts = []
    for pair in range(2):
        for shard in range(2):
            win = get(1 + 4 * pair + shard)
            width = win.shape[1]
            for col in range(0, width, step):
                act = gelu(mm(a_ref[...], win[:, col : col + step], 1, 0))
                start = (2 * pair + shard) * width + col
                act_ref[:, start : start + step] = act.astype(BF)
        wout = jnp.concatenate([get(3 + 4 * pair)[...], get(4 + 4 * pair)[...]], axis=0)
        parts.append(mm(act_ref[:, 2 * pair * width : 2 * (pair + 1) * width], wout, 1, 0))
    out_ref[...] = get(9)[...] - (parts[0] + parts[1])
    out_store()


def rebuild_step(where, x, y, weights, after):
    tokens, hidden = x.dims
    width = weights[0].dims[1]
    scratch = [pltpu.VMEM((tokens, hidden), BF), pltpu.VMEM((tokens, 4 * width), BF)]
    return kernel_call(
        rebuild_body, "rebuild", where, [x, *weights, y], [Out(x.dims, F32)], scratch, after, flops=16 * tokens * hidden * width
    )


def attn_out_body(get, put, scratch):
    near = mm(get(0)[...], jnp.concatenate([get(1)[...], get(2)[...]], axis=0), 1, 0)
    far = mm(get(3)[...], jnp.concatenate([get(4)[...], get(5)[...]], axis=0), 1, 0)
    put[0][0][...] = get(6)[...] - (near + far)
    put[0][1]()


def attn_out_step(where, y, heads, heads_far, wo, after):
    ins = [In(heads), wo[0], wo[1], In(heads_far), wo[2], wo[3], y]
    flops = 4 * y.dims[0] * y.dims[1] * heads.shape[1]
    return kernel_call(attn_out_body, "attn_out", where, ins, [Out(y.dims, F32)], (), after, flops=flops)


def dw_body(half, wide, add, names, get, put, scratch):
    tile = 256

    def rows_of(name):
        return jnp.concatenate([get(names[name, seq])[...] for seq in range(2)], axis=0)

    def turned(name, start):
        return jnp.concatenate([get(names[name, seq])[:, start : start + tile] for seq in range(2)], axis=0).T

    def emit(slot, row, value):
        rows = slice(row, row + value.shape[0])
        if add:
            value = value + get(names["recv", slot])[rows, :]
        put[slot][0][rows, :] = value
        put[slot][1](rows)

    def picked(moved):
        return moved[:wide] if half == 0 else moved[tile - wide :]

    start = 0 if half == 0 else 2 * wide - tile
    for slot, (left, right) in enumerate((("a_mlp", "dh"), ("act", "d_two"))):
        others = rows_of(right)
        for row in range(0, put[slot][0].shape[0], tile):
            emit(slot, row, mm(turned(left, row), others, 1, 0))
    others = rows_of("a_attn")
    for part in range(3):
        emit(2, part * wide, mm(picked(turned("dqkv", part * 2 * wide + start)), others, 1, 0))
    emit(3, 0, mm(picked(turned("heads", start)), rows_of("d_one"), 1, 0))


def dw_step(where, half, attn_parts, mlp_parts, layer, recv, stacks, layers, after):
    loads = [("a_mlp", 0, None), ("dh", 1, half), ("act", 2, half), ("d_two", 3, None)]
    names, ins = {}, []

    def put_in(key, item):
        names[key] = len(ins)
        ins.append(item)

    tokens, hidden = attn_parts[0][0].shape
    width = mlp_parts[0][1][0].shape[1]
    wide = attn_parts[0][2].shape[1] // 2
    dims = [(hidden, width), (width, hidden), (3 * wide, hidden), (wide, hidden)]
    for key, slot, part in loads:
        for seq in range(2):
            arr = mlp_parts[seq][slot]
            put_in((key, seq), In(arr if part is None else arr[part]))
        if recv is not None and key in ("dh", "d_two"):
            put_in(("recv", 0 if key == "dh" else 1), In(recv[0 if key == "dh" else 1]))
    for slot, key in enumerate(("a_attn", "dqkv", "heads", "d_one")):
        for seq in range(2):
            put_in((key, seq), In(attn_parts[seq][slot]))
        if recv is not None and key in ("dqkv", "d_one"):
            put_in(("recv", 2 if key == "dqkv" else 3), In(recv[2 if key == "dqkv" else 3]))
    if recv is None:
        outs = [Out(dim, F32) for dim in dims]
    else:
        outs = [
            Out(dim, F32, (layers,) + dim, lambda ref, first: ref.at[layer], None if stacks is None else stacks[slot])
            for slot, dim in enumerate(dims)
        ]
    flops = 4 * tokens * hidden * (4 * wide + 2 * width)
    return kernel_call(
        functools.partial(dw_body, half, wide, recv is not None, names),
        "dw_theirs" if recv is None else "dw_mine",
        where,
        ins,
        outs,
        (),
        after,
        flops=flops,
    )


def settle_body(get, put, scratch):
    for seq in range(2):
        put[seq][0][...] = get(3 * seq)[...] + (get(3 * seq + 1)[...].astype(F32) + get(3 * seq + 2)[...].astype(F32))
        put[seq][1]()


def whole_body(get, put, scratch):
    for seq in range(2):
        put[0][1](src=get(seq), at=lambda ref, first, seq=seq: ref.at[first + seq])
        put[0][1](src=get(2 + seq), at=lambda ref, first, seq=seq: ref.at[2 - first + seq])


def solution(mesh):
    act_spec = P("dp", None, None)
    saved_spec = P(None, "dp", None, None)
    weight_specs = (P(None, None, None, "tp", None), P(None, "tp", None, None), P(None, None, "tp"), P(None, "tp", None))
    grad_specs = (P("dp", None, None, "tp", None), P("dp", "tp", None, None), P("dp", None, "tp"), P("dp", "tp", None))
    across = [(0, 2), (2, 0), (1, 3), (3, 1)]
    partner = [(0, 1), (1, 0), (2, 3), (3, 2)]

    def per_device(y_one, y_two, dy_one, dy_two, saved_one, saved_two, w_qkv, w_o, w_in, w_out):
        layers, pairs = w_qkv.shape[0], saved_one.shape[0]
        tokens, hidden = y_one.shape[1:]
        dims = (tokens, hidden)
        group = lax.axis_index("dp")
        where = jnp.stack([2 * lax.rem(lax.axis_index("tp"), 2), group]).astype(jnp.int32)

        def far(value):
            return lax.ppermute(value, "tp", across)

        def near(value):
            return lax.ppermute(value, "tp", partner)

        wq_t = jnp.transpose(w_qkv, (0, 2, 3, 4, 1)).reshape(layers, -1, hidden)
        wo_r = w_o.reshape(layers, -1, hidden)
        wide = wo_r.shape[1]
        top = layers - 1

        def at_layer(arr, layer):
            return In(arr, arr.shape[1:], lambda ref, first: ref.at[layer])

        def at_seq(arr, seq):
            return In(arr, dims, lambda ref, first: ref.at[first + seq])

        def at_pair_seq(arr, pair, seq):
            return In(arr, dims, lambda ref, first: ref.at[pair, first + seq])

        top_in, top_out = near(w_in[top]), near(w_out[top])
        far_w = {}

        def fetch_far(layer, token=None):
            pick = group if token is None else lax.optimization_barrier((group, token))[0]
            sent = jnp.where(pick == 0, w_in[layer], w_out[layer])
            one = far(sent)
            two = lax.ppermute(one, "dp", [(0, 1), (1, 0)])
            one_par, two_par = near(one), near(two)
            far_w[layer] = [In(one, other=two), In(one_par, other=two_par), In(two, other=one), In(two_par, other=one_par)]

        fetch_far(top)
        wq_par, wo_par, win_par, wout_par = near(wq_t), near(wo_r), near(w_in), near(w_out)
        attn_w = [[at_layer(arr, layer) for arr in (wq_t, wq_par, wo_r, wo_par)] for layer in range(layers)]
        mlp_w = [[at_layer(arr, layer) for arr in (w_in, w_out, win_par, wout_par)] for layer in range(layers)]
        mlp_w[top][2:] = [In(top_in), In(top_out)]

        last = [()]

        def run(step, *args):
            made = step(where, *args, last[0])
            last[0] = (made[0],)
            return made

        d_one = [Cotangent(at_seq(dy_one, seq), dims) for seq in range(2)]
        d_two = [Cotangent(at_seq(dy_two, seq), dims) for seq in range(2)]
        in_one, in_two, x_two = {}, {}, {}
        for seq in range(2):
            in_one[pairs, seq], in_two[pairs, seq] = at_seq(y_one, seq), at_seq(y_two, seq)
            for pair in range(pairs):
                in_one[pair, seq] = at_pair_seq(saved_one, pair, seq)
                in_two[pair, seq] = at_pair_seq(saved_two, pair, seq)

        attn_parts, mlp_parts, acc = {}, {}, {}

        def attn(layer, seq):
            x = In(x_two[layer, seq]) if layer % 2 == 0 else in_two[layer // 2, seq]
            part, a, dqkv, heads = run(attn_step, x, d_one[seq], attn_w[layer])
            attn_parts[layer, seq] = (a, dqkv, heads, d_one[seq].bf.arr)
            return part, far(part)

        def mlp(layer, seq):
            reversible = layer % 2 == 0
            part, a, act_own, act_par, dh_own, dh_par = run(
                mlp_step, in_one[layer // 2, seq], d_two[seq], mlp_w[layer], acc.get(seq) if reversible else None, reversible
            )
            mlp_parts[layer, seq] = (a, (dh_own, dh_par), (act_own, act_par), d_two[seq].bf.arr)
            acc[seq] = None if reversible else part
            return part, (far(part) if reversible else None)

        def rebuild(layer, seq):
            own_in, own_out, par_in, par_out = mlp_w[layer]
            weights = [own_in, par_in, own_out, par_out] + far_w[layer]
            x_two[layer, seq] = run(rebuild_step, in_one[layer // 2, seq], in_two[layer // 2, seq], weights)[0]

        stacks, sent = [None], {}

        def grads(layer):
            parts = [[table[layer, seq] for seq in range(2)] for table in (attn_parts, mlp_parts)]
            made = run(dw_step, 1, *parts, layer, None, None, layers)
            sent[layer] = (parts, [near(value) for value in made])

        def grads_end(layer):
            parts, recv = sent[layer]
            stacks[0] = run(dw_step, 0, *parts, layer, recv, stacks[0], layers)

        def whole(own):
            ins = [In(value) for value in own] + [In(near(value)) for value in own]
            out = Out((8, 128), F32, (4,) + dims)
            return run(lambda where, after: kernel_call(whole_body, "whole", where, ins, [out], (), after))[0]

        for seq in range(2):
            d_one[seq].add(*mlp(top, seq))
        for seq in range(2):
            rebuild(top, seq)
        for pair in reversed(range(pairs + 1)):
            layer = 2 * pair
            if pair:
                fetch_far(layer - 2, last[0][0])
            two = {}
            for seq in range(2):
                d_two[seq].add(*attn(layer, seq))
                if pair:
                    two[seq] = attn(layer - 1, seq)
            if pair == 0:
                break
            for seq in range(2):
                mlp(layer - 1, seq)
                rebuild(layer - 2, seq)
                if seq == 0:
                    grads(layer)
                d_two[seq].add(*two[seq])
                d_one[seq].add(*mlp(layer - 2, seq))
            grads(layer - 1)
            grads_end(layer)
            grads_end(layer - 1)
        wo_own, wo_near = wo_r[0], wo_par[0]
        wo_all = [In(value) for value in (wo_own, wo_near, far(wo_own), far(wo_near))]
        grads(0)
        x_two_all = whole([x_two[0, seq] for seq in range(2)])
        d_one_all = whole([d_one[seq].value.arr for seq in range(2)])
        grads_end(0)
        x_one = []
        for seq in range(2):
            heads = attn_parts[0, seq][2]
            x_one.append(run(attn_out_step, in_one[0, seq], heads, far(heads), wo_all)[0])
        ins = [item for seq in range(2) for item in (d_two[seq].value, *d_two[seq].pending)]
        settled = run(
            lambda where, after: kernel_call(settle_body, "settle", where, ins, [Out(dims, F32), Out(dims, F32)], (), after)
        )
        x_one_all, d_two_all = whole(x_one), whole(settled)
        dwin, dwout, dwq, dwo = stacks[0]
        dwq = jnp.transpose(dwq.reshape((layers,) + w_qkv.shape[2:] + (hidden,)), (0, 4, 1, 2, 3))
        return x_one_all, x_two_all, d_one_all, d_two_all, dwq, dwo.reshape(w_o.shape), dwin, dwout

    return jax.shard_map(
        per_device,
        mesh=mesh,
        in_specs=(act_spec,) * 4 + (saved_spec,) * 2 + weight_specs,
        out_specs=(act_spec,) * 4 + grad_specs,
        check_vma=False,
    )
```

```python
import functools
import math

import jax
import jax.numpy as jnp
from jax import lax
from jax.experimental import pallas as pl
from jax.experimental.pallas import tpu as pltpu
from jax.sharding import PartitionSpec as P

EPS = 1e-6
BF = jnp.bfloat16
F32 = jnp.float32
GELU_A = math.sqrt(2.0 / math.pi)
GELU_B = 0.044715 * GELU_A
GELU_D = 3.0 * GELU_B
HALF = 0.5
SCALE = 0.125
ROWS = 32
LANES = 128
WIDE = 2 * LANES
COPIES = 64
AHEAD = 4
PAIR = (0, 1)
CONTRACT = {"nn": ((1,), (0,)), "nt": ((1,), (1,)), "tn": ((0,), (0,))}


def mm(lhs, rhs, kind="nn"):
    return lax.dot_general(lhs, rhs, (CONTRACT[kind], ((), ())), preferred_element_type=F32)


def rows_cat(parts):
    return jnp.concatenate(parts, axis=0)


class In:
    def __init__(self, arr, dims=None, at=None, other=None):
        self.arr, self.other = arr, other
        self.dims = tuple(dims or arr.shape)
        self.at = at or (lambda ref, first: ref)


class Out:
    def __init__(self, dims, dtype, full=None, at=None, into=None):
        self.dims, self.dtype = tuple(dims), dtype
        self.full = tuple(full or dims)
        self.at = at or (lambda ref, first: ref)
        self.into = into


class Moves:
    def __init__(self, sems):
        self.sems, self.used, self.open, self.loads, self.started = sems, 0, [], [], 0

    def sem(self):
        self.used += 1
        return self.sems.at[self.used - 1]

    def load(self, sources, pick, dst):
        sem = self.sem()
        copies = [pltpu.make_async_copy(src, dst, sem) for src in sources]

        def start():
            if len(copies) == 1:
                copies[0].start()
            else:
                pl.when(pick == 0)(copies[0].start)
                pl.when(pick != 0)(copies[1].start)

        self.loads.append([start, copies[0], dst])

    def get(self, idx):
        while self.started < min(idx + AHEAD, len(self.loads)):
            self.loads[self.started][0]()
            self.started += 1
        _, copy, dst = self.loads[idx]
        if copy is not None:
            copy.wait()
            self.loads[idx][1] = None
        return dst

    def store(self, src, dst):
        copy = pltpu.make_async_copy(src, dst, self.sem())
        copy.start()
        self.open.append(copy)

    def finish(self):
        for copy in self.open:
            copy.wait()


def kernel_call(body, name, where, ins, outs, scratch=(), after=(), flops=0):
    arrays, slots, alias = [where], [], {}
    for item in ins:
        slots.append([len(arrays)] + ([len(arrays) + 1] if item.other is not None else []))
        arrays += [item.arr] + ([item.other] if item.other is not None else [])
    for idx, item in enumerate(outs):
        if item.into is not None:
            alias[len(arrays)] = idx
            arrays.append(item.into)
    arrays += [value for value in after if all(value is not item.into for item in outs)]

    def wrapped(*refs):
        where_ref, out_refs = refs[0], refs[len(arrays) : len(arrays) + len(outs)]
        rest = refs[len(arrays) + len(outs) :]
        in_bufs, out_bufs = rest[: len(ins)], rest[len(ins) : len(ins) + len(outs)]
        moves = Moves(rest[-1])
        first, pick = where_ref[0], where_ref[1]
        for idx, item in enumerate(ins):
            moves.load([item.at(refs[slot], first) for slot in slots[idx]], pick, in_bufs[idx])

        def storer(idx):
            def store(rows=None, src=None, at=None):
                dst = (at or outs[idx].at)(out_refs[idx], first)
                src = out_bufs[idx] if src is None else src
                if rows is not None:
                    src, dst = src.at[rows], dst.at[rows]
                moves.store(src, dst)

            return store

        body(moves.get, [(out_bufs[idx], storer(idx)) for idx in range(len(outs))], rest[len(ins) + len(outs) : -1])
        moves.finish()

    anywhere = pl.BlockSpec(memory_space=pl.ANY)
    moved = sum(math.prod(item.dims) * item.arr.dtype.itemsize for item in ins)
    moved += sum(math.prod(item.dims) * jnp.dtype(item.dtype).itemsize for item in outs)
    return pl.pallas_call(
        wrapped,
        out_shape=[jax.ShapeDtypeStruct(item.full, item.dtype) for item in outs],
        in_specs=[pl.BlockSpec(memory_space=pltpu.SMEM)] + [anywhere] * (len(arrays) - 1),
        out_specs=[anywhere] * len(outs),
        scratch_shapes=[pltpu.VMEM(item.dims, item.arr.dtype) for item in ins]
        + [pltpu.VMEM(item.dims, item.dtype) for item in outs]
        + list(scratch)
        + [pltpu.SemaphoreType.DMA((COPIES,))],
        input_output_aliases=alias,
        compiler_params=pltpu.CompilerParams(vmem_limit_bytes=60 << 20),
        cost_estimate=pl.CostEstimate(flops=flops, bytes_accessed=moved, transcendentals=0),
        name=name,
    )(*arrays)


def inv_rms(x):
    return lax.rsqrt(jnp.mean(x * x, axis=-1, keepdims=True) + EPS)


def pull_norm(x, grad):
    inv = inv_rms(x)
    return inv * (grad - x * (inv * inv * jnp.mean(grad * x, axis=-1, keepdims=True)))


def gelu(hid):
    half = HALF * hid
    return half + half * jnp.tanh(hid * (GELU_A + GELU_B * (hid * hid)))


def gelu_and_slope(hid):
    sq = hid * hid
    tanh = jnp.tanh(hid * (GELU_A + GELU_B * sq))
    half = HALF * hid
    act = half + half * tanh
    slope = (HALF + HALF * tanh) + (half - half * (tanh * tanh)) * (GELU_A + GELU_D * sq)
    return act, slope


class Queue:
    def __init__(self, get, put):
        self.get_idx, self.put_idx, self.get, self.put = 0, 0, get, put

    def next_in(self):
        self.get_idx += 1
        return functools.partial(self.get, self.get_idx - 1)

    def next_out(self):
        self.put_idx += 1
        return self.put[self.put_idx - 1]


def read_cotangent(mode, queue):
    first = queue.next_in()
    if mode == "have":
        return first()
    bf_ref, bf_store = queue.next_out()
    total = first()[...]
    if mode == "add":
        mine, recv = queue.next_in()(), queue.next_in()()
        total = total + (mine[...].astype(F32) + recv[...].astype(F32))
        full_ref, full_store = queue.next_out()
        full_ref[...] = total
        full_store()
    bf_ref[...] = total.astype(BF)
    bf_store()
    return bf_ref


def attn_block(queue, x_ref, d_of, scratch):
    t_ref, t_store = queue.next_out()
    a_ref, a_store = queue.next_out()
    dqkv_ref, dqkv_store = queue.next_out()
    o_ref, o_store = queue.next_out()
    qkv_ref, do_ref, s_ref, dp_ref, pb_ref, ds_ref = scratch
    tokens = x_ref.shape[0]
    x = x_ref[...]
    a_ref[...] = (x * inv_rms(x)).astype(BF)
    a_store()
    halves = [queue.next_in()() for _ in PAIR]
    wide = halves[0].shape[0] // 3
    both = wide + wide
    w_all = rows_cat([ref[part * wide : (part + 1) * wide, :] for part in range(3) for ref in halves])
    qkv = mm(a_ref[...], w_all, "nt")
    qkv_ref[:, :both] = qkv[:, :both].astype(BF) * jnp.asarray(SCALE, BF)
    qkv_ref[:, both:] = qkv[:, both:].astype(BF)
    d_ref = d_of()
    do_ref[...] = mm(d_ref[...], rows_cat([queue.next_in()()[...] for _ in PAIR]), "nt").astype(BF)
    lane = lax.broadcasted_iota(jnp.int32, (tokens, LANES), 1)
    low_lanes = lane < LANES // 2
    for start in range(0, both, LANES):
        cols, k_cols, v_cols = (slice(base + start, base + start + LANES) for base in (0, both, both + both))
        q_two, k_two, v_two, do_two = qkv_ref[:, cols], qkv_ref[:, k_cols], qkv_ref[:, v_cols], do_ref[:, cols]
        zero = jnp.zeros_like(q_two)
        sums = []
        for head in PAIR:

            def only(value):
                return jnp.where(low_lanes, value, zero) if head == 0 else jnp.where(low_lanes, zero, value)

            s_ref[head] = mm(only(q_two), k_two, "nt")
            dp_ref[head] = mm(only(do_two), v_two, "nt")
            for row in range(0, tokens, ROWS):
                rows = slice(row, row + ROWS)
                scores = s_ref[head, rows, :]
                d_probs = dp_ref[head, rows, :]
                exps = jnp.exp(scores - jnp.max(scores, axis=-1, keepdims=True))
                probs = exps * (1.0 / jnp.sum(exps, axis=-1, keepdims=True))
                pb_ref[head, rows, :] = probs.astype(BF)
                ds_ref[head, rows, :] = (probs * (d_probs - jnp.sum(d_probs * probs, axis=-1, keepdims=True))).astype(BF)
            probs, d_scores = pb_ref[head], ds_ref[head]
            sums.append((mm(probs, v_two), mm(d_scores, k_two), mm(d_scores, q_two, "tn"), mm(probs, do_two, "tn")))
        heads, d_q, d_k, d_v = (jnp.where(low_lanes, low, high) for low, high in zip(*sums))
        o_ref[:, cols] = heads.astype(BF)
        dqkv_ref[:, cols] = (d_q * SCALE).astype(BF)
        dqkv_ref[:, k_cols] = d_k.astype(BF)
        dqkv_ref[:, v_cols] = d_v.astype(BF)
    o_store()
    dqkv_store()
    t_ref[...] = pull_norm(x_ref[...], mm(dqkv_ref[...], w_all)).astype(BF)
    t_store()


def attn_body(mode, count, get, put, scratch):
    queue = Queue(get, put)
    made = []

    def d_of():
        if not made:
            made.append(read_cotangent(mode, queue))
        return made[0]

    for _ in range(count):
        attn_block(queue, queue.next_in()(), d_of, scratch)


def cotangent_outs(mode, dims):
    return {"have": [], "cast": [Out(dims, BF)], "add": [Out(dims, BF), Out(dims, F32)]}[mode]


def attn_step(where, mode, d_in, blocks, after):
    dims = blocks[0][0].dims
    tokens, hidden = dims
    wide = blocks[0][1][2].dims[0]
    both = wide + wide
    ins, outs = [], []
    for idx, (x, (wq_own, wq_par, wo_own, wo_par)) in enumerate(blocks):
        ins += [x, wq_own, wq_par] + (d_in if idx == 0 else []) + [wo_own, wo_par]
        outs += [Out(dims, BF), Out(dims, BF), Out((tokens, 3 * both), BF), Out((tokens, both), BF)]
        outs += cotangent_outs(mode, dims) if idx == 0 else []
    scratch = [pltpu.VMEM((tokens, 3 * both), BF), pltpu.VMEM((tokens, both), BF)]
    scratch += [pltpu.VMEM((2, tokens, tokens), dtype) for dtype in (F32, F32, BF, BF)]
    flops = len(blocks) * (14 * tokens * hidden * both + 12 * tokens * tokens * 4 * both)
    made = kernel_call(functools.partial(attn_body, mode, len(blocks)), "attn_back", where, ins, outs, scratch, after, flops=flops)
    extra = len(cotangent_outs(mode, dims))
    parts = [made[:4]] + ([made[4 + extra :]] if len(blocks) > 1 else [])
    return made, parts, made[4 : 4 + extra]


def mlp_block(queue, x_ref, a_ref, d_ref):
    wins, wouts, dhs = [], [], []
    for _ in PAIR:
        win, wout = queue.next_in()(), queue.next_in()()
        (act_ref, act_store), (dh_ref, dh_store) = queue.next_out(), queue.next_out()
        wins.append(win)
        dhs.append(dh_ref)
        for col in range(0, win.shape[1], WIDE):
            cols = slice(col, col + WIDE)
            act, slope = gelu_and_slope(mm(a_ref[...], win[:, cols]))
            act_ref[:, cols] = act.astype(BF)
            dh_ref[:, cols] = (mm(d_ref[...], wout[cols, :], "nt") * slope).astype(BF)
        act_store()
        dh_store()
    side = [jnp.concatenate([ref[...] for ref in refs], axis=1) for refs in (dhs, wins)]
    return pull_norm(x_ref[...], mm(*side, "nt"))


def mlp_body(blocks, get, put, scratch):
    queue = Queue(get, put)
    t_ref, t_store = queue.next_out()
    a_ref, a_store = queue.next_out()
    x_ref = queue.next_in()()
    x = x_ref[...]
    a_ref[...] = (x * inv_rms(x)).astype(BF)
    a_store()
    value = queue.next_in()()[...]
    total = None
    for block in range(blocks):
        bf_ref, bf_store = queue.next_out()
        if blocks > 1:
            mine, recv = queue.next_in()(), queue.next_in()()
            value = value + (mine[...].astype(F32) + recv[...].astype(F32))
            if block == 0:
                scratch[0][...] = value
            else:
                full_ref, full_store = queue.next_out()
                full_ref[...] = value
                full_store()
        bf_ref[...] = value.astype(BF)
        bf_store()
        part = mlp_block(queue, x_ref, a_ref, bf_ref)
        if block + 1 < blocks:
            scratch[1][...] = part
            value = scratch[0][...]
        else:
            total = part if blocks == 1 else scratch[1][...] + part
    t_ref[...] = total.astype(BF)
    t_store()


def mlp_step(where, x, value, blocks, after):
    dims = x.dims
    tokens, hidden = dims
    ins, outs = [x, value], [Out(dims, BF), Out(dims, BF)]
    for idx, (pair, weights) in enumerate(blocks):
        ins += [In(part) for part in pair]
        outs.append(Out(dims, BF))
        if idx:
            outs.append(Out(dims, F32))
        width = weights[0].dims[1]
        ins += weights
        outs += [Out((tokens, width), BF)] * 4
    scratch = [pltpu.VMEM(dims, F32)] * 2 if len(blocks) > 1 else []
    flops = 12 * tokens * hidden * width * len(blocks)
    made = kernel_call(functools.partial(mlp_body, len(blocks)), "mlp_back", where, ins, outs, scratch, after, flops=flops)
    a, rest, parts = made[1], made[2:], []
    for idx in range(len(blocks)):
        bf, rest = rest[0], rest[1:]
        if idx:
            full, rest = rest[0], rest[1:]
        parts.append((a, (rest[0], rest[2], rest[1], rest[3]), bf))
        rest = rest[4:]
    return made, parts, (In(full) if len(blocks) > 1 else None)


def rebuild_body(get, put, scratch):
    a_ref, act_ref = scratch
    queue = Queue(get, put)
    tokens = put[0][0].shape[0]
    for seq in PAIR:
        x = queue.next_in()()[...]
        a_ref[seq * tokens : (seq + 1) * tokens, :] = (x * inv_rms(x)).astype(BF)
    parts = []
    for pair in PAIR:
        wouts = []
        for shard in PAIR:
            win = queue.next_in()()
            width = win.shape[1]
            for col in range(0, width, WIDE):
                start = shard * width + col
                act_ref[:, start : start + WIDE] = gelu(mm(a_ref[...], win[:, col : col + WIDE])).astype(BF)
        wout = rows_cat([queue.next_in()()[...] for _ in PAIR])
        made = mm(act_ref[...], wout)
        if pair == 0:
            for seq in PAIR:
                put[seq][0][...] = made[seq * tokens : (seq + 1) * tokens]
        else:
            for seq in PAIR:
                out_ref, store = put[seq]
                out_ref[...] = queue.next_in()()[...] - (out_ref[...] + made[seq * tokens : (seq + 1) * tokens])
                store()


def rebuild_step(where, xs, ys, near_w, far_w, after):
    tokens, hidden = xs[0].dims
    width = near_w[0].dims[1]
    scratch = [pltpu.VMEM((2 * tokens, hidden), BF), pltpu.VMEM((2 * tokens, 2 * width), BF)]
    outs = [Out(xs[0].dims, F32)] * 2
    flops = 32 * tokens * hidden * width
    return kernel_call(rebuild_body, "rebuild", where, [*xs, *near_w, *far_w, *ys], outs, scratch, after, flops=flops)


def attn_out_body(get, put, scratch):
    queue = Queue(get, put)
    sums = []
    for _ in PAIR:
        heads = queue.next_in()()[...]
        sums.append(mm(heads, rows_cat([queue.next_in()()[...] for _ in PAIR])))
    put[0][0][...] = queue.next_in()()[...] - (sums[0] + sums[1])
    put[0][1]()


def attn_out_step(where, y, heads, heads_far, wo, after):
    ins = [In(heads), wo[0], wo[1], In(heads_far), wo[2], wo[3], y]
    flops = 4 * y.dims[0] * y.dims[1] * heads.shape[1]
    return kernel_call(attn_out_body, "attn_out", where, ins, [Out(y.dims, F32)], (), after, flops=flops)


def dw_body(half, wide, names, add, get, put, scratch):
    def rows_of(name):
        return rows_cat([get(names[name, seq])[...] for seq in PAIR])

    def turned(name, start):
        return rows_cat([get(names[name, seq])[:, start : start + WIDE] for seq in PAIR]).T

    def emit(slot, row, value):
        rows = slice(row, row + value.shape[0])
        ref, store = put[slot]
        if add:
            value = value + get(names["recv", slot])[rows, :]
        ref[rows, :] = value
        store(rows)

    def picked(moved):
        return moved[:wide] if half == 0 else moved[WIDE - wide :]

    start = 0 if half == 0 else wide + wide - WIDE
    for slot, (left, right) in enumerate((("a_mlp", "dh"), ("act", "d_two"))):
        others = rows_of(right)
        for row in range(0, put[slot][0].shape[0], WIDE):
            emit(slot, row, mm(turned(left, row), others))
    others = rows_of("a_attn")
    for part in range(3):
        emit(2, part * wide, mm(picked(turned("dqkv", part * 2 * wide + start)), others))
    emit(3, 0, mm(picked(turned("heads", start)), rows_of("d_one")))


def dw_step(where, half, attn_parts, mlp_parts, layer, recv, stacks, layers, after):
    tables = {
        "dh": [part[1][2 + half] for part in mlp_parts],
        "a_mlp": [part[0] for part in mlp_parts],
        "d_two": [part[2] for part in mlp_parts],
        "act": [part[1][half] for part in mlp_parts],
        "a_attn": [part[1] for part in attn_parts],
        "dqkv": [part[2] for part in attn_parts],
        "d_one": [part[4] for part in attn_parts],
        "heads": [part[3] for part in attn_parts],
    }
    names, ins = {}, []
    for idx, (key, arrs) in enumerate(tables.items()):
        for seq in PAIR:
            names[key, seq] = len(ins)
            ins.append(In(arrs[seq]))
        if idx % 2 and recv is not None:
            names["recv", idx // 2] = len(ins)
            ins.append(In(recv[idx // 2]))
    tokens, hidden = tables["a_attn"][0].shape
    width = tables["dh"][0].shape[1]
    wide = tables["heads"][0].shape[1] // 2
    dims = [(hidden, width), (width, hidden), (3 * wide, hidden), (wide, hidden)]
    if recv is None:
        outs = [Out(dim, F32) for dim in dims]
    else:
        into = stacks or [None] * 4
        outs = [Out(dim, F32, (layers,) + dim, lambda ref, first: ref.at[layer], arr) for dim, arr in zip(dims, into)]
    body = functools.partial(dw_body, half, wide, names, recv is not None)
    name = "dw_mine" if half == 0 else "dw_theirs"
    return kernel_call(body, name, where, ins, outs, (), after, flops=4 * tokens * hidden * (4 * wide + 2 * width))


def settle_body(get, put, scratch):
    for seq in PAIR:
        value, mine, recv = (get(3 * seq + idx)[...] for idx in range(3))
        put[seq][0][...] = value + (mine.astype(F32) + recv.astype(F32))
        put[seq][1]()


def whole_body(get, put, scratch):
    for seq in PAIR:
        put[0][1](src=get(seq), at=lambda ref, first, seq=seq: ref.at[first + seq])
        put[0][1](src=get(2 + seq), at=lambda ref, first, seq=seq: ref.at[2 - first + seq])


def solution(mesh):
    act_spec = P("dp", None, None)
    saved_spec = P(None, "dp", None, None)
    weight_specs = (P(None, None, None, "tp", None), P(None, "tp", None, None), P(None, None, "tp"), P(None, "tp", None))
    grad_specs = (P("dp", None, None, "tp", None), P("dp", "tp", None, None), P("dp", None, "tp"), P("dp", "tp", None))
    across = [(dev, dev ^ 2) for dev in range(4)]
    partner = [(dev, dev ^ 1) for dev in range(4)]

    def per_device(y_one, y_two, dy_one, dy_two, saved_one, saved_two, w_qkv, w_o, w_in, w_out):
        layers, pairs = w_qkv.shape[0], saved_one.shape[0]
        dims = y_one.shape[1:]
        hidden = dims[1]
        group = lax.axis_index("dp")
        where = jnp.stack([2 * lax.rem(lax.axis_index("tp"), 2), group]).astype(jnp.int32)
        last = [()]

        def run(step, *args):
            made = step(where, *args, last[0])
            last[0] = ((made[0] if isinstance(made, list) else made[0][0]),)
            return made

        def hold(value):
            return lax.optimization_barrier((value, last[0][0]))[0]

        def far(value):
            return lax.ppermute(value, "tp", across)

        def near(value):
            return lax.ppermute(value, "tp", partner)

        wq_t = jnp.transpose(w_qkv, (0, 2, 3, 4, 1)).reshape(layers, -1, hidden)
        wo_r = w_o.reshape(layers, -1, hidden)
        top = layers - 1

        def at_layer(arr, layer):
            return In(arr, arr.shape[1:], lambda ref, first: ref.at[layer])

        def at_seq(arr, seq, pair=None):
            return In(arr, dims, lambda ref, first: ref.at[first + seq] if pair is None else ref.at[pair, first + seq])

        far_w = {}

        def far_start(layer):
            pick = hold(group) if last[0] else group
            far_w[layer] = [far(jnp.where(pick == 0, w_in[layer], w_out[layer]))]

        def far_next(layer):
            one = hold(far_w[layer][0])
            far_w[layer] = [one, lax.ppermute(one, "dp", [(0, 1), (1, 0)]), near(one)]

        def far_end(layer):
            one, two, one_par = far_w[layer]
            two_par = near(hold(two))
            far_w[layer] = [In(one, other=two), In(one_par, other=two_par), In(two, other=one), In(two_par, other=one_par)]

        def attn_w(layer):
            return [at_layer(arr, layer) for arr in (wq_t, par["wq"], wo_r, par["wo"])]

        def mlp_w(layer):
            return [at_layer(arr, layer) for arr in (w_in, w_out, par["win"], par["wout"])]

        def x_of(layer, seq):
            if layer % 2 == 0:
                return In(x_two[layer][seq])
            return in_two[layer // 2][seq]

        in_one = [[at_seq(saved_one, seq, pair) for seq in PAIR] for pair in range(pairs)] + [[at_seq(y_one, seq) for seq in PAIR]]
        in_two = [[at_seq(saved_two, seq, pair) for seq in PAIR] for pair in range(pairs)] + [[at_seq(y_two, seq) for seq in PAIR]]
        x_two, par = {}, {}
        d_one = [at_seq(dy_one, seq) for seq in PAIR]
        d_two = [at_seq(dy_two, seq) for seq in PAIR]
        one_new, two_new = [[], []], [[], []]
        attn_parts, mlp_parts = {}, {}
        d_bf = [None, None]

        def attn(blocks, seq):
            if one_new[seq]:
                mode, d_in = "add", [d_one[seq], *one_new[seq]]
            else:
                mode, d_in = "have", [In(d_bf[seq])]
            _, parts, extra = run(attn_step, mode, d_in, [(x_of(layer, seq), attn_w(layer)) for layer in blocks])
            if extra:
                d_bf[seq], d_one[seq] = extra[0], In(extra[1])
            one_new[seq] = []
            for layer, part in zip(blocks, parts):
                attn_parts[layer, seq] = (*part, d_bf[seq])
            return [(part[0], far(part[0])) for part in parts]

        def mlp(blocks, seq):
            news = two_new[seq] if len(blocks) > 1 else [()]
            made, parts, full = run(
                mlp_step, in_one[blocks[0] // 2][seq], d_two[seq], [(pair, weights) for pair, weights in zip(news, map(mlp_w, blocks))]
            )
            if full is not None:
                d_two[seq] = full
            for layer, part in zip(blocks, parts):
                mlp_parts[layer, seq] = part
            one_new[seq] = [In(made[0]), In(far(made[0]))]

        def rebuild(layer):
            own_in, own_out, par_in, par_out = mlp_w(layer)
            pair = layer // 2
            x_two[layer] = run(rebuild_step, in_one[pair], in_two[pair], [own_in, par_in, own_out, par_out], far_w[layer])

        stacks, sent = [None], {}

        def grads(layer):
            parts = [[table[layer, seq] for seq in PAIR] for table in (attn_parts, mlp_parts)]
            made = run(dw_step, 1, *parts, layer, None, None, layers)
            sent[layer] = (parts, [near(value) for value in made])

        def grads_end(layer):
            parts, recv = sent[layer]
            stacks[0] = run(dw_step, 0, *parts, layer, recv, stacks[0], layers)

        def whole(own):
            ins = [In(value) for value in own] + [In(near(value)) for value in own]
            out = Out((8, LANES), F32, (4,) + dims)
            return run(lambda where, after: kernel_call(whole_body, "whole", where, ins, [out], (), after))[0]

        pair_order = list(reversed(range(1, pairs + 1)))
        par_top = (near(w_in[top]), near(w_out[top]))
        far_start(top)
        mlp_top = [at_layer(w_in, top), at_layer(w_out, top), In(par_top[0]), In(par_top[1])]
        for seq in PAIR:
            made, parts, _ = run(mlp_step, in_one[pairs][seq], d_two[seq], [((), mlp_top)])
            mlp_parts[top, seq] = parts[0]
            one_new[seq] = [In(made[0]), In(far(made[0]))]
            if seq == 0:
                par["wq"], par["wo"] = near(hold(wq_t)), near(hold(wo_r))
        far_next(top)
        second = [attn([top - 1], 0)[0], None]
        par["win"], par["wout"] = near(hold(w_in)), near(hold(w_out))
        second[1] = attn([top - 1], 1)[0]
        far_end(top)
        rebuild(top)
        far_start(top - 2)
        two_new = [[attn([top], seq)[0], second[seq]] for seq in PAIR]
        late = None
        for pair in pair_order:
            layer = 2 * pair
            if layer != top:
                for seq in PAIR:
                    two_new[seq] = attn([layer, layer - 1], seq)
                    if seq == 0:
                        far_next(layer - 2)
            else:
                far_next(layer - 2)
            grads(layer)
            far_end(layer - 2)
            if late is not None:
                grads_end(late)
            rebuild(layer - 2)
            mlp([layer - 1, layer - 2], 0)
            grads_end(layer)
            mlp([layer - 1, layer - 2], 1)
            if layer > 2:
                far_start(layer - 4)
            grads(layer - 1)
            late = layer - 1
        ends = [attn([0], seq)[0] for seq in PAIR]
        wo_all = [In(value) for value in (wo_r[0], par["wo"][0], far(wo_r[0]), far(par["wo"][0]))]
        grads_end(late)
        grads(0)
        x_two_all = whole(x_two[0])
        d_one_all = whole([value.arr for value in d_one])
        x_one = []
        for seq in PAIR:
            heads = attn_parts[0, seq][3]
            x_one.append(run(attn_out_step, in_one[0][seq], heads, far(heads), wo_all)[0])
        ins = [item for seq in PAIR for item in (d_two[seq], In(ends[seq][0]), In(ends[seq][1]))]
        settled = run(lambda where, after: kernel_call(settle_body, "settle", where, ins, [Out(dims, F32)] * 2, (), after))
        grads_end(0)
        x_one_all, d_two_all = whole(x_one), whole(settled)
        dwin, dwout, dwq, dwo = stacks[0]
        dwq = jnp.transpose(dwq.reshape((layers,) + w_qkv.shape[2:] + (hidden,)), (0, 4, 1, 2, 3))
        return x_one_all, x_two_all, d_one_all, d_two_all, dwq, dwo.reshape(w_o.shape), dwin, dwout

    return jax.shard_map(
        per_device,
        mesh=mesh,
        in_specs=(act_spec,) * 4 + (saved_spec,) * 2 + weight_specs,
        out_specs=(act_spec,) * 4 + grad_specs,
        check_vma=False,
    )
```
